256 devices in a mesh: section: 4 (over x), dp: 64 (over y, z, core).
Axes of the slice: x: 4, y: 4, z: 8, core: 2. Of those that a mesh axis runs over, the one named last changes fastest.
Arguments:
- acts: bfloat16 [4, 16384, 2560], P('section', 'dp'), may hold values from -6 to 6
- gates: bfloat16 [4, 16384, 1280], P('section', 'dp'), may hold values from -6 to 6
- w_value: bfloat16 [4, 2560, 1280], P('section', 'dp'), may hold values from -0.125 to 0.125
- w_out: bfloat16 [4, 2560, 1280], P('section', 'dp'), may hold values from -0.125 to 0.125
- residual_error: bfloat16 [4, 163840, 1280], P('section', 'dp'), may hold values from -48 to 48
- grad_top: bfloat16 [16384, 2560], P('dp'), may hold values from -6 to 6
- warm_factor: float32 [4, 4, 1280], P('section'), may hold values from -6 to 6
Outputs:
- grad_in: bfloat16 [4, 16384, 2560], P('section', 'dp')
- basis_out: float32 [4, 4, 2560], P('section')
- right_out: float32 [4, 4, 1280], P('section')
The draws below stay inside these ranges and needn't reach their ends.
All inputs are finite; a program needn't handle non-finite values.
Results may differ from the reference program's by a relative error of at most 0.009.
Values may be sent and summed in bfloat16 or wider, within the bound.
A program may use at most 128 MiB of HBM per device.

```python
import math
import jax
import jax.numpy as jnp
from jax import lax

D = 2560
C = 1280
RANK = 4
TOKENS = 16384
N_SECTION = 4
N_DP = 64


def steps_of(key, extent, pieces, least, largest):
    def one(dim, parts):
        steps = jax.random.uniform(jax.random.fold_in(jax.random.fold_in(key, 6), dim), (parts,), jnp.float32, least / len(pieces), largest / len(pieces))
        return jnp.repeat(jnp.exp(steps), extent[dim] // parts).reshape((-1,) + (1,) * (len(extent) - dim - 1))

    gain = one(*pieces[0])
    for cut in pieces[1:]:
        gain = gain * one(*cut)
    return gain


def bell_draw(key, shape, spread, most, shards=(), held_as=jnp.bfloat16):
    array = spread * jax.random.normal(key, shape, jnp.float32)
    if shards:
        array = array * steps_of(key, shape, shards, -0.22, 0.18)
    return jnp.clip(array, -most, most).astype(held_as)


def setup_inputs(seed: int = 0) -> dict:
    arg_keys = jax.random.split(jax.random.key(seed), 8)
    return {
        "acts": bell_draw(arg_keys[0], (N_SECTION, TOKENS, D), 1.0, 6.0, ((0, 4), (1, 64))),
        "gates": bell_draw(arg_keys[1], (N_SECTION, TOKENS, C), 1.0, 6.0, ((0, 4), (1, 64))),
        "w_value": bell_draw(arg_keys[2], (N_SECTION, D, C), D ** -0.5, 0.125, ((0, 4), (1, 64))),
        "w_out": bell_draw(arg_keys[3], (N_SECTION, D, C), D ** -0.5, 0.125, ((0, 4), (1, 64))),
        "residual_error": bell_draw(arg_keys[4], (N_SECTION, N_DP * D, C), 8.0, 48.0, ((0, 4), (1, 64))),
        "grad_top": bell_draw(arg_keys[5], (TOKENS, D), 1.0, 6.0, ((0, 64),)),
        "warm_factor": bell_draw(arg_keys[6], (N_SECTION, RANK, C), 1.0, 6.0, ((0, 4),), jnp.float32),
    }


HIGHEST_PRECISION = lax.Precision.HIGHEST

def orthonormal(vectors):
    result = []
    for column in range(vectors.shape[0]):
        current = vectors[column]
        for previous in result:
            current = current - jnp.mean(current * previous) * previous
        current = current / jnp.sqrt(jnp.mean(current * current) + 1e-06)
        result.append(current)
    return jnp.stack(result)

def reference(acts, gates, w_value, w_out, residual_error, grad_top, warm_factor):
    arriving = grad_top
    passed_list = []
    basis_list = []
    right_list = []
    for layer_index in reversed(range(N_SECTION)):
        hidden = jnp.dot(arriving, w_out[layer_index], preferred_element_type=jnp.float32)
        value_grad = (hidden * gates[layer_index].astype(jnp.float32)).astype(jnp.bfloat16)
        back_term = lax.dot_general(value_grad, w_value[layer_index], (((1,), (1,)), ((), ())), preferred_element_type=jnp.float32)
        passed = (arriving.astype(jnp.float32) + back_term).astype(jnp.bfloat16)
        inputs_wide = acts[layer_index].astype(jnp.float32)
        grads_wide = value_grad.astype(jnp.float32)
        error_sum = lax.optimization_barrier(jnp.sum(residual_error[layer_index].astype(jnp.float32).reshape(N_DP, D, C), axis=0))
        warm_start = warm_factor[layer_index]
        projected = jnp.dot(grads_wide, warm_start.T, precision=HIGHEST_PRECISION)
        factor = jnp.dot(projected.T, inputs_wide, precision=HIGHEST_PRECISION) + jnp.dot(warm_start, error_sum.T, precision=HIGHEST_PRECISION)
        basis_rows = orthonormal(factor)
        mapped = jnp.dot(inputs_wide, basis_rows.T, precision=HIGHEST_PRECISION)
        second = jnp.dot(mapped.T, grads_wide, precision=HIGHEST_PRECISION) + jnp.dot(basis_rows, error_sum, precision=HIGHEST_PRECISION)
        second = second / math.sqrt(TOKENS * D)
        passed_list.insert(0, passed)
        basis_list.insert(0, basis_rows)
        right_list.insert(0, second)
        arriving = passed
    return (jnp.stack(passed_list), jnp.stack(basis_list), jnp.stack(right_list))
```

```python
import functools
import math

import jax
import jax.numpy as jnp
from jax import lax
from jax.experimental import pallas as pl
from jax.experimental.pallas import tpu as pltpu
from jax.sharding import Mesh
from jax.sharding import PartitionSpec as P

MESH = pl.DeviceIdType.MESH
F32, BF16 = jnp.float32, jnp.bfloat16
RANK = 4
GROUP = 8
NZ = 8


def parts_of(v):
    high = v.astype(BF16)
    rest = v - high.astype(F32)
    mid = rest.astype(BF16)
    low = (rest - mid.astype(F32)).astype(BF16)
    stack = [high.astype(F32), mid.astype(F32), low.astype(F32), jnp.zeros_like(v)]
    return jnp.concatenate(stack, axis=0).astype(BF16)


def joined(t):
    return t[0:RANK] + (t[RANK : 2 * RANK] + t[2 * RANK : 3 * RANK])


def dot_nn(a, b):
    return lax.dot_general(a, b, (((1,), (0,)), ((), ())), preferred_element_type=F32)


def dot_nt(a, b):
    return lax.dot_general(a, b, (((1,), (1,)), ((), ())), preferred_element_type=F32)


def orthonormal(vectors):
    result = []
    width = vectors.shape[1]
    for j in range(RANK):
        current = vectors[j : j + 1]
        for previous in result:
            current = current - (jnp.sum(current * previous, axis=1, keepdims=True) / width) * previous
        norm = jnp.sqrt(jnp.sum(current * current, axis=1, keepdims=True) / width + 1e-06)
        current = current / norm
        result.append(current)
    return jnp.concatenate(result, axis=0)


def all_reduced(value, width, src, rs, zs, out, send, recv):
    y, z, core = lax.axis_index("y"), lax.axis_index("z"), lax.axis_index("core")
    me = y * 2 + core
    total = value.shape[1]
    for piece in range(GROUP):
        lo, hi = piece * width, min((piece + 1) * width, total)
        if hi > lo:
            src[piece, :, 0 : hi - lo] = value[:, lo:hi]
        if hi - lo < width:
            src[piece, :, max(hi - lo, 0) : width] = jnp.zeros((RANK, width - max(hi - lo, 0)), F32)
    rs[me] = src[me]

    def to_group(step, from_ref, dst, phase):
        peer = lax.rem(me + step, GROUP)
        return pltpu.make_async_remote_copy(
            src_ref=from_ref(peer), dst_ref=dst.at[me],
            send_sem=send.at[phase, step], recv_sem=recv.at[phase, step],
            device_id={"y": peer // 2, "core": lax.rem(peer, 2)}, device_id_type=MESH)

    def to_line(step):
        peer = lax.rem(z + step, NZ)
        return pltpu.make_async_remote_copy(
            src_ref=zs.at[z], dst_ref=zs.at[z],
            send_sem=send.at[1, step], recv_sem=recv.at[1, step],
            device_id={"z": peer}, device_id_type=MESH)

    first = [to_group(s, lambda p: src.at[p], rs, 0) for s in range(1, GROUP)]
    for c in first:
        c.start()
    for c in first:
        c.wait()
    acc = rs[0]
    for i in range(1, GROUP):
        acc = acc + rs[i]
    zs[z] = acc
    second = [to_line(s) for s in range(1, NZ)]
    for c in second:
        c.start()
    for c in second:
        c.wait()
    acc = zs[0]
    for i in range(1, NZ):
        acc = acc + zs[i]
    out[me] = acc
    third = [to_group(s, lambda p: out.at[me], out, 2) for s in range(1, GROUP)]
    for c in third:
        c.start()
    for c in third:
        c.wait()
    pieces = [out[i] for i in range((total + width - 1) // width)]
    return jnp.concatenate(pieces, axis=1)[:, :total]


def entry_barrier():
    y, z, core = lax.axis_index("y"), lax.axis_index("z"), lax.axis_index("core")
    me = y * 2 + core
    barrier = pltpu.get_barrier_semaphore()
    for step in range(1, GROUP):
        peer = lax.rem(me + step, GROUP)
        pl.semaphore_signal(barrier, inc=1, device_id={"y": peer // 2, "core": lax.rem(peer, 2)}, device_id_type=MESH)
    for step in range(1, NZ):
        pl.semaphore_signal(barrier, inc=1, device_id={"z": lax.rem(z + step, NZ)}, device_id_type=MESH)
    pl.semaphore_wait(barrier, GROUP + NZ - 2)


def powersgd_kernel(scale, acts, vg, err, warm, basis_out, right_out,
                    src1, rs1, zs1, out1, send1, recv1, src2, rs2, zs2, out2, send2, recv2):
    entry_barrier()
    w = parts_of(warm[...])
    projected = joined(dot_nt(w, vg[...]))
    width = acts.shape[1]
    step = 512
    p = parts_of(projected)
    cols = []
    for at in range(0, width, step):
        t = dot_nn(p, acts[:, at : at + step]) + dot_nt(w, err[at : at + step, :])
        cols.append(joined(t))
    factor = all_reduced(jnp.concatenate(cols, axis=1), 384, src1, rs1, zs1, out1, send1, recv1)
    basis = orthonormal(factor)
    basis_out[...] = basis
    b = parts_of(basis)
    m = parts_of(joined(dot_nt(b, acts[...])))
    t = dot_nn(m, vg[...]) + dot_nn(b, err[...])
    right = all_reduced(joined(t), 256, src2, rs2, zs2, out2, send2, recv2)
    right_out[...] = right / scale


def ar_scratch(width):
    return [
        pltpu.VMEM((GROUP, RANK, width), F32),
        pltpu.VMEM((GROUP, RANK, width), F32),
        pltpu.VMEM((NZ, RANK, width), F32),
        pltpu.VMEM((GROUP, RANK, width), F32),
        pltpu.SemaphoreType.DMA((3, 8)),
        pltpu.SemaphoreType.DMA((3, 8)),
    ]


def powersgd(acts, vg, err, warm, scale):
    vmem = pl.BlockSpec(memory_space=pltpu.VMEM)
    return pl.pallas_call(
        functools.partial(powersgd_kernel, scale),
        out_shape=(
            jax.ShapeDtypeStruct((RANK, acts.shape[1]), F32),
            jax.ShapeDtypeStruct((RANK, vg.shape[1]), F32),
        ),
        in_specs=[vmem] * 4,
        out_specs=(vmem, vmem),
        scratch_shapes=ar_scratch(384) + ar_scratch(256),
        compiler_params=pltpu.CompilerParams(
            collective_id=1, has_side_effects=True, vmem_limit_bytes=40 << 20),
    )(acts, vg, err, warm)


MICRO = 4
DP = ("y", "z", "core")


def in_one_piece(arrays, axis, dim, along):
    both = jnp.concatenate(arrays, axis=along)
    whole, at, finished = (lax.all_gather(both, axis, axis=dim, tiled=True), 0, [])
    for a in arrays:
        finished.append(lax.slice_in_dim(whole, at, at + a.shape[along], axis=along))
        at += a.shape[along]
    return tuple(finished)


def shifted(value, axis, by):
    peers = lax.axis_size(axis)
    pairs = [(i, i + by) for i in range(peers) if 0 <= i + by < peers]
    return lax.ppermute(value, axis, pairs)


def local(acts, gates, w_value, w_out, residual_error, grad_top, warm_factor):
    value_full, out_full = in_one_piece((w_value[0], w_out[0]), DP, 0, 1)
    section_count = lax.axis_size("section")
    section_index = lax.axis_index("section")
    inputs = acts[0]
    gate_rows = gates[0]
    row_count = inputs.shape[0]
    model_width = inputs.shape[1]
    block_rows = row_count // MICRO
    value_grads = jnp.zeros((row_count, gate_rows.shape[1]), jnp.bfloat16)
    passed_rows = jnp.zeros((row_count, model_width), jnp.bfloat16)
    incoming = jnp.zeros((block_rows, model_width), jnp.bfloat16)
    turn_count = MICRO + section_count - 1
    for step_index in range(turn_count):
        micro_index = step_index - (section_count - 1 - section_index)
        active = (micro_index >= 0) & (micro_index < MICRO)
        offset = jnp.clip(micro_index, 0, MICRO - 1) * block_rows
        top_rows = lax.dynamic_slice_in_dim(grad_top, offset, block_rows, 0)
        arriving = jnp.where(section_index == section_count - 1, top_rows, incoming)
        gate_block = lax.dynamic_slice_in_dim(gate_rows, offset, block_rows, 0)
        hidden = jnp.dot(arriving, out_full, preferred_element_type=jnp.float32)
        value_grad = (hidden * gate_block.astype(jnp.float32)).astype(jnp.bfloat16)
        back_term = lax.dot_general(
            value_grad, value_full, (((1,), (1,)), ((), ())), preferred_element_type=jnp.float32
        )
        passed = (arriving.astype(jnp.float32) + back_term).astype(jnp.bfloat16)
        value_grads = jnp.where(
            active, lax.dynamic_update_slice_in_dim(value_grads, value_grad, offset, 0), value_grads
        )
        passed_rows = jnp.where(
            active, lax.dynamic_update_slice_in_dim(passed_rows, passed, offset, 0), passed_rows
        )
        if step_index + 1 < turn_count:
            incoming = shifted(passed, "section", -1)
    scale = math.sqrt(row_count * lax.axis_size(DP) * model_width)
    basis_rows, second = powersgd(inputs, value_grads, residual_error[0], warm_factor[0], scale)
    return (passed_rows[None], basis_rows[None], second[None])


def solution(mesh):
    finer = Mesh(
        mesh.devices.reshape(mesh.shape["section"], 4, 8, 2), ("section", "y", "z", "core")
    )
    return jax.shard_map(
        local,
        mesh=finer,
        in_specs=(
            P("section", DP, None),
            P("section", DP, None),
            P("section", DP, None),
            P("section", DP, None),
            P("section", DP, None),
            P(DP, None),
            P("section", None, None),
        ),
        out_specs=(P("section", DP, None), P("section", None, None), P("section", None, None)),
        check_vma=False,
    )
```
